32 devices in a mesh: groups: 2 (over x), tensor: 16 (over z, y, core).
Axes of the slice: x: 2, y: 2, z: 4, core: 2. Of those that a mesh axis runs over, the one named last changes fastest.
Arguments:
- video_state: float32 [128, 4096], P(('groups', 'tensor')), parts along dimension 0, may hold values from -54 to 54
- audio_state: float32 [128, 2048], P(('groups', 'tensor')), parts along dimension 0, may hold values from -54 to 54
- video_modulation: float32 [12, 4096], P('groups'), parts along dimension 0, may hold values from -3 to 3
- audio_modulation: float32 [12, 2048], P('groups'), parts along dimension 0, may hold values from -3 to 3
- video_query: bfloat16 [4096, 2048], P(None, 'tensor'), may hold values from -0.09375 to 0.09375
- audio_keyval: bfloat16 [2048, 2, 2048], P(None, None, 'tensor'), may hold values from -0.125 to 0.125
- video_output: bfloat16 [2048, 4096], P('tensor'), may hold values from -0.125 to 0.125
- audio_query: bfloat16 [2048, 2048], P(None, 'tensor'), may hold values from -0.125 to 0.125
- video_keyval: bfloat16 [4096, 2, 2048], P(None, None, 'tensor'), may hold values from -0.09375 to 0.09375
- audio_output: bfloat16 [2048, 2048], P('tensor'), may hold values from -0.125 to 0.125
- video_expand: bfloat16 [4096, 16384], P(None, 'tensor'), may hold values from -0.09375 to 0.09375
- video_shrink: bfloat16 [16384, 4096], P('tensor'), may hold values from -0.046875 to 0.046875
- audio_expand: bfloat16 [2048, 8192], P(None, 'tensor'), may hold values from -0.125 to 0.125
- audio_shrink: bfloat16 [8192, 2048], P('tensor'), may hold values from -0.0625 to 0.0625
Outputs:
- video_next: float32 [128, 4096], P(('groups', 'tensor')), parts along dimension 0
- audio_next: float32 [128, 2048], P(('groups', 'tensor')), parts along dimension 0
The draws below stay inside these ranges and needn't reach their ends.
There are 2 independent parts, one for each index of `groups`. The reference program is written for one: setup_inputs(seed, part) draws one part's arguments, and reference() takes and returns one part's arrays. A program takes and returns all parts, laid end to end along the dimension named above; an argument that names none is the same for every part. Nothing has to cross between parts.
All inputs are finite; a program needn't handle non-finite values.
Results may differ from the reference program's by a relative error of at most 0.0029.
Values may be sent and summed in bfloat16 or wider, within the bound.
A program may use at most 64 MiB of HBM per device.

```python
import math
import jax
import jax.numpy as jnp
from jax import lax

DV = 4096
FFV = 16384
DA = 2048
FFA = 8192
HEADS = 32
HEAD_DIM = 64
INNER = 2048
TV = 64
TA = 64


def state_draw(key, rows, width):
    row_key, column_key, base_key = jax.random.split(key, 3)
    row_scale = jnp.exp(jax.random.uniform(row_key, (rows, 1), jnp.float32, math.log(0.3), math.log(3.0)))
    column_scale = jnp.exp(jax.random.uniform(column_key, (1, width), jnp.float32, math.log(0.3), math.log(3.0)))
    base = jnp.clip(jax.random.normal(base_key, (rows, width), jnp.float32), -6.0, 6.0)
    return base * row_scale * column_scale


def draw_video_state(key, part):
    return state_draw(jax.random.fold_in(key, 3), TV, DV)


def draw_audio_state(key, part):
    return state_draw(jax.random.fold_in(key, 7), TA, DA)


def levels(own_key, extent, cuts, smallest, high):
    factor_of, own = 1.0, jax.random.fold_in(own_key, 6)
    for dim, blocks in cuts:
        draws = jnp.exp(jax.random.uniform(jax.random.fold_in(own, dim), (blocks,), jnp.float32, smallest / len(cuts), high / len(cuts)))
        factor_of = factor_of * jnp.repeat(draws, extent[dim] // blocks).reshape([-1 if axis == dim else 1 for axis in range(len(extent))])
    return factor_of


def gaussian(stream_key, extent, scale, most, pieces=(), dtype=jnp.bfloat16):
    entries = scale * jax.random.normal(stream_key, extent, jnp.float32)
    if pieces:
        entries = entries * levels(stream_key, extent, pieces, -0.22, 0.18)
    return jnp.clip(entries, -most, most).astype(dtype)


def setup_inputs(seed: int = 0, part: int = 0) -> dict:
    seeds = jax.random.split(jax.random.key(seed), 15)
    part_splits = jax.random.split(jax.random.fold_in(seeds[14], part), 15)
    return {
        "video_state": draw_video_state(jax.random.fold_in(jax.random.fold_in(seeds[14], part), 71), part),
        "audio_state": draw_audio_state(jax.random.fold_in(jax.random.fold_in(seeds[14], part), 71), part),
        "video_modulation": gaussian(part_splits[2], (6, DV), 0.5, 3.0, (), jnp.float32),
        "audio_modulation": gaussian(part_splits[3], (6, DA), 0.5, 3.0, (), jnp.float32),
        "video_query": gaussian(seeds[4], (DV, INNER), DV ** -0.5, 0.09375, ((1, 16),)),
        "audio_keyval": gaussian(seeds[5], (DA, 2, INNER), DA ** -0.5, 0.125, ((2, 16),)),
        "video_output": gaussian(seeds[6], (INNER, DV), INNER ** -0.5, 0.125, ((0, 16),)),
        "audio_query": gaussian(seeds[7], (DA, INNER), DA ** -0.5, 0.125, ((1, 16),)),
        "video_keyval": gaussian(seeds[8], (DV, 2, INNER), DV ** -0.5, 0.09375, ((2, 16),)),
        "audio_output": gaussian(seeds[9], (INNER, DA), INNER ** -0.5, 0.125, ((0, 16),)),
        "video_expand": gaussian(seeds[10], (DV, FFV), DV ** -0.5, 0.09375, ((1, 16),)),
        "video_shrink": gaussian(seeds[11], (FFV, DV), FFV ** -0.5, 0.046875, ((0, 16),)),
        "audio_expand": gaussian(seeds[12], (DA, FFA), DA ** -0.5, 0.125, ((1, 16),)),
        "audio_shrink": gaussian(seeds[13], (FFA, DA), FFA ** -0.5, 0.0625, ((0, 16),)),
    }


epsilon = 1e-06

def modulate(states, modulation, first):
    normed = states * lax.rsqrt(lax.optimization_barrier(jnp.mean(states * states, axis=-1, keepdims=True)) + epsilon)
    return (normed * (1.0 + modulation[first + 1]) + modulation[first]).astype(jnp.bfloat16)

def head_normalize(tensor):
    values = tensor.astype(jnp.float32).reshape(tensor.shape[0], HEADS, HEAD_DIM)
    return values * lax.rsqrt(lax.optimization_barrier(jnp.mean(values * values, axis=-1, keepdims=True)) + epsilon)

def attend(query_rows, source_rows, query_weight, keyval_weight, output_weight):
    queries = jnp.dot(query_rows, query_weight, preferred_element_type=jnp.float32).astype(jnp.bfloat16)
    flat_weight = keyval_weight.reshape(keyval_weight.shape[0], 2 * INNER)
    keyvals = jnp.dot(source_rows, flat_weight, preferred_element_type=jnp.float32).astype(jnp.bfloat16)
    key_part = keyvals[:, :INNER]
    value_part = keyvals[:, INNER:].astype(jnp.float32).reshape(source_rows.shape[0], HEADS, HEAD_DIM)
    query_hat = head_normalize(queries).astype(jnp.bfloat16).astype(jnp.float32)
    key_hat = head_normalize(key_part).astype(jnp.bfloat16).astype(jnp.float32)
    scores = jnp.einsum('qhd,khd->hqk', query_hat, key_hat) * HEAD_DIM ** (-0.5)
    expo = jnp.exp(scores)
    weights = (expo / lax.optimization_barrier(jnp.sum(expo, axis=-1, keepdims=True))).astype(jnp.bfloat16).astype(jnp.float32)
    mixed = jnp.einsum('hqk,khd->qhd', weights, value_part).astype(jnp.bfloat16)
    mixed = mixed.reshape(query_rows.shape[0], INNER)
    return jnp.dot(mixed, output_weight, preferred_element_type=jnp.float32)

def feed_forward(inputs, expand, shrink):
    hidden = jnp.dot(inputs, expand, preferred_element_type=jnp.float32)
    hidden = jax.nn.gelu(hidden, approximate=True).astype(jnp.bfloat16)
    return jnp.dot(hidden, shrink, preferred_element_type=jnp.float32)

def reference(video_state, audio_state, video_modulation, audio_modulation, video_query, audio_keyval, video_output, audio_query, video_keyval, audio_output, video_expand, video_shrink, audio_expand, audio_shrink):
    video_normed = modulate(video_state, video_modulation, 0)
    audio_normed = modulate(audio_state, audio_modulation, 0)
    video_mid = video_state + video_modulation[2] * attend(video_normed, audio_normed, video_query, audio_keyval, video_output)
    audio_mid = audio_state + audio_modulation[2] * attend(audio_normed, video_normed, audio_query, video_keyval, audio_output)
    video_inner = modulate(video_mid, video_modulation, 3)
    audio_inner = modulate(audio_mid, audio_modulation, 3)
    video_next = video_mid + video_modulation[5] * feed_forward(video_inner, video_expand, video_shrink)
    audio_next = audio_mid + audio_modulation[5] * feed_forward(audio_inner, audio_expand, audio_shrink)
    return (video_next, audio_next)
```

```python
import functools

import jax
import jax.numpy as jnp
from jax import lax
from jax.experimental import pallas as pl
from jax.experimental.pallas import tpu as pltpu
from jax.sharding import PartitionSpec as P

HEAD_DIM = 64


epsilon = 1e-06


def partner(block, axis, distance):
    count = lax.axis_size(axis)
    route = []
    for low in range(count):
        high = low | 1 << distance
        if high != low and high < count:
            route += [(low, high), (high, low)]
    return lax.ppermute(block, axis, route)


def modulate(states, modulation, first):
    normed = states * lax.rsqrt(jnp.mean(states * states, axis=-1, keepdims=True) + epsilon)
    return (normed * (1.0 + modulation[first + 1]) + modulation[first]).astype(jnp.bfloat16)


def head_normalize(tensor):
    values = tensor.astype(jnp.float32)
    return (values * lax.rsqrt(jnp.mean(values * values, axis=-1, keepdims=True) + epsilon)).astype(
        jnp.bfloat16
    )


def softmax_weights(scores):
    expo = jnp.exp(scores)
    return (expo / jnp.sum(expo, axis=-1, keepdims=True)).astype(jnp.bfloat16)


def local_heads(queries, key_part, value_part):
    query_count, width = queries.shape
    source_count = key_part.shape[0]
    head_count = width // HEAD_DIM
    query_hat = head_normalize(queries.reshape(query_count, head_count, HEAD_DIM))
    key_hat = head_normalize(key_part.reshape(source_count, head_count, HEAD_DIM))
    scores = jnp.einsum(
        "qhd,khd->hqk", query_hat, key_hat, preferred_element_type=jnp.float32
    ) * HEAD_DIM ** (-0.5)
    weights = softmax_weights(scores)
    values = value_part.reshape(source_count, head_count, HEAD_DIM)
    mixed = jnp.einsum("hqk,khd->qhd", weights, values, preferred_element_type=jnp.float32)
    return mixed.astype(jnp.bfloat16).reshape(query_count, width)


def project_attend(query_rows, source_rows, query_weight, keyval_weight):
    width = query_weight.shape[1]
    queries = jnp.dot(query_rows, query_weight, preferred_element_type=jnp.float32).astype(
        jnp.bfloat16
    )
    flat_weight = keyval_weight.reshape(keyval_weight.shape[0], 2 * width)
    keyvals = jnp.dot(source_rows, flat_weight, preferred_element_type=jnp.float32).astype(
        jnp.bfloat16
    )
    key_part = keyvals[:, :width]
    value_part = keyvals[:, width:]
    if width >= HEAD_DIM:
        return local_heads(queries, key_part, value_part)
    query_float = queries.astype(jnp.float32)
    key_float = key_part.astype(jnp.float32)
    query_square = jnp.sum(query_float * query_float, axis=1, keepdims=True)
    key_square = jnp.sum(key_float * key_float, axis=1, keepdims=True)
    other_query, other_key = partner((query_square, key_square), "tensor", 0)
    query_hat = (query_float * lax.rsqrt((query_square + other_query) / HEAD_DIM + epsilon)).astype(
        jnp.bfloat16
    )
    key_hat = (key_float * lax.rsqrt((key_square + other_key) / HEAD_DIM + epsilon)).astype(
        jnp.bfloat16
    )
    partial_scores = jnp.einsum("qd,kd->qk", query_hat, key_hat, preferred_element_type=jnp.float32)
    other_scores = partner(partial_scores, "tensor", 0)
    scores = (partial_scores + other_scores) * HEAD_DIM ** (-0.5)
    weights = softmax_weights(scores)
    return jnp.dot(weights, value_part, preferred_element_type=jnp.float32).astype(jnp.bfloat16)


def output_rows(mixed, weight):
    return jnp.dot(mixed, weight, preferred_element_type=jnp.float32)


def feed_rows(inputs, expand, shrink):
    hidden = jnp.dot(inputs, expand, preferred_element_type=jnp.float32)
    hidden = jax.nn.gelu(hidden, approximate=True).astype(jnp.bfloat16)
    return jnp.dot(hidden, shrink, preferred_element_type=jnp.float32)


def on_device(
    video_state,
    audio_state,
    video_modulation,
    audio_modulation,
    video_query,
    audio_keyval,
    video_output,
    audio_query,
    video_keyval,
    audio_output,
    video_expand,
    video_shrink,
    audio_expand,
    audio_shrink,
):
    video_count = video_state.shape[0]
    audio_own = modulate(audio_state, audio_modulation, 0)
    video_whole = lax.all_gather(video_state, "tensor", axis=0, tiled=True)
    video_normed = modulate(video_whole, video_modulation, 0)
    audio_normed = lax.all_gather(audio_own, "tensor", axis=0, tiled=True)
    video_mixed = project_attend(video_normed, audio_normed, video_query, audio_keyval)
    audio_mixed = project_attend(audio_normed, video_normed, audio_query, video_keyval)
    audio_term = lax.psum_scatter(
        output_rows(audio_mixed, audio_output), "tensor", scatter_dimension=0, tiled=True
    )
    audio_mid = audio_state + audio_modulation[2] * audio_term
    audio_inner_own = modulate(audio_mid, audio_modulation, 3)
    partial_term = jnp.dot(video_mixed, video_output, preferred_element_type=jnp.float32)
    full_term = lax.psum(partial_term, "tensor")
    video_mid_whole = video_whole + video_modulation[2] * full_term
    video_inner = modulate(video_mid_whole, video_modulation, 3)
    first_row = lax.axis_index("tensor") * video_count
    video_mid = lax.dynamic_slice_in_dim(video_mid_whole, first_row, video_count, 0)
    audio_inner = lax.all_gather(audio_inner_own, "tensor", axis=0, tiled=True)
    video_feed = lax.psum_scatter(
        feed_rows(video_inner, video_expand, video_shrink),
        "tensor",
        scatter_dimension=0,
        tiled=True,
    )
    audio_feed = lax.psum_scatter(
        feed_rows(audio_inner, audio_expand, audio_shrink),
        "tensor",
        scatter_dimension=0,
        tiled=True,
    )
    video_next = video_mid + video_modulation[5] * video_feed
    audio_next = audio_mid + audio_modulation[5] * audio_feed
    return (video_next, audio_next)


VMEM_BYTES = 66_000_000
WEIGHT_BYTES = 40 << 20


def matmul_to(lhs_ref, weight_ref, tile, emit):
    def body(i, carry):
        columns = pl.ds(pl.multiple_of(i * tile, tile), tile)
        emit(
            columns,
            jnp.dot(lhs_ref[...], weight_ref[:, columns], preferred_element_type=jnp.float32),
        )
        return carry

    lax.fori_loop(0, weight_ref.shape[1] // tile, body, 0)


class Stream:
    names = ("own", "slots", "wide", "whole", "other", "paired", "sums", "terms", "total")

    @staticmethod
    def scratch(count, rows, width):
        chips = count // 2
        return [
            pltpu.VMEM((rows, width), jnp.bfloat16),
            pltpu.VMEM((count, rows, width), jnp.bfloat16),
            pltpu.VMEM((chips, 2 * rows, width), jnp.float32),
            pltpu.VMEM((count * rows, width), jnp.bfloat16),
            pltpu.VMEM((chips, rows, width), jnp.bfloat16),
            pltpu.VMEM((chips, rows, width), jnp.bfloat16),
            pltpu.VMEM((chips, rows, width), jnp.bfloat16),
            pltpu.VMEM((chips, rows, width), jnp.bfloat16),
            pltpu.VMEM((rows, width), jnp.float32),
            pltpu.SemaphoreType.DMA((2 * chips,)),
            pltpu.SemaphoreType.DMA((count,)),
            pltpu.SemaphoreType.DMA((chips + 1,)),
            pltpu.SemaphoreType.DMA((chips + 1,)),
        ]

    def __init__(self, refs, count):
        for name, ref in zip(self.names, refs):
            setattr(self, name, ref)
        self.gather_send, self.gather_recv, self.scatter_send, self.scatter_recv = refs[len(self.names):]
        self.count, self.chips = count, count // 2
        self.rows = self.own.shape[0]
        self.me = lax.axis_index("tensor")
        self.chip, self.core = self.me // 2, self.me % 2
        self.mate = self.chip * 2 + (1 - self.core)

    def distant(self, step):
        return lax.rem(self.chip + step, self.chips)

    def to_mate(self, slot, source, send):
        return pltpu.make_async_remote_copy(
            src_ref=source,
            dst_ref=self.slots.at[slot],
            send_sem=self.gather_send.at[send],
            recv_sem=self.gather_recv.at[slot],
            device_id={"tensor": self.mate},
            device_id_type=pl.DeviceIdType.MESH,
        )

    def to_chip(self, step):
        return pltpu.make_async_remote_copy(
            src_ref=self.own,
            dst_ref=self.slots.at[self.me],
            send_sem=self.gather_send.at[step],
            recv_sem=self.gather_recv.at[self.me],
            device_id={"tensor": self.distant(step) * 2 + self.core},
            device_id_type=pl.DeviceIdType.MESH,
        )

    def keep(self):
        return pltpu.make_async_copy(self.own, self.slots.at[self.me], self.gather_recv.at[self.me])

    def gather_start(self):
        for step in range(self.chips - 1, 0, -1):
            self.to_chip(step).start()
        self.to_mate(self.me, self.own, 0).start()
        self.keep().start()

    def arrived(self, slot):
        pltpu.make_async_copy(self.slots.at[slot], self.slots.at[slot], self.gather_recv.at[slot]).wait()

    def gather_forward(self):
        for step in range(1, self.chips):
            slot = self.distant(step) * 2 + self.core
            self.arrived(slot)
            self.to_mate(slot, self.slots.at[slot], self.chips + step).start()

    def gather_finish(self):
        self.keep().wait()
        for step in range(self.chips):
            self.arrived(self.distant(step) * 2 + 1 - self.core)

        def widen(chip, carry):
            self.wide[chip, : self.rows, :] = self.slots[2 * chip].astype(jnp.float32)
            self.wide[chip, self.rows :, :] = self.slots[2 * chip + 1].astype(jnp.float32)
            return carry

        lax.fori_loop(0, self.chips, widen, 0)
        self.whole[...] = self.wide[...].reshape(self.whole.shape).astype(jnp.bfloat16)

    def gather_drain(self):
        for step in range(1, self.chips):
            slot = self.distant(step) * 2 + self.core
            self.to_chip(step).wait_send()
            self.to_mate(slot, self.slots.at[slot], self.chips + step).wait_send()
        self.to_mate(self.me, self.own, 0).wait_send()

    def emit(self, columns, product):
        self.wide[:, :, columns] = product.reshape(self.chips, 2 * self.rows, product.shape[1])

    def swap(self):
        return pltpu.make_async_remote_copy(
            src_ref=self.other,
            dst_ref=self.paired,
            send_sem=self.scatter_send.at[self.chips],
            recv_sem=self.scatter_recv.at[self.chips],
            device_id={"tensor": self.mate},
            device_id_type=pl.DeviceIdType.MESH,
        )

    def halves(self, chip):
        rows = self.wide[chip]
        low, high = rows[: self.rows], rows[self.rows :]
        first = self.core == 0
        return jnp.where(first, low, high), jnp.where(first, high, low)

    def scatter_start(self):
        def body(chip, carry):
            self.other[chip] = self.halves(chip)[1].astype(jnp.bfloat16)
            return carry

        lax.fori_loop(0, self.chips, body, 0)
        self.swap().start()

    def term(self, step):
        goal = self.distant(step)
        return pltpu.make_async_remote_copy(
            src_ref=self.sums.at[goal],
            dst_ref=self.terms.at[self.chip],
            send_sem=self.scatter_send.at[step],
            recv_sem=self.scatter_recv.at[self.chip],
            device_id={"tensor": goal * 2 + self.core},
            device_id_type=pl.DeviceIdType.MESH,
        )

    def scatter_send_on(self):
        self.swap().wait()
        for step in range(1, self.chips):
            goal = self.distant(step)
            self.sums[goal] = (
                self.halves(goal)[0] + self.paired[goal].astype(jnp.float32)
            ).astype(jnp.bfloat16)
            self.term(step).start()
        self.total[...] = self.halves(self.chip)[0] + self.paired[self.chip].astype(jnp.float32)

    def scatter_finish(self):
        for step in range(1, self.chips):
            source = self.distant(step)
            pltpu.make_async_copy(
                self.terms.at[source], self.terms.at[source], self.scatter_recv.at[source]
            ).wait()
            self.total[...] += self.terms[source].astype(jnp.float32)
        for step in range(1, self.chips):
            self.term(step).wait_send()
        return self.total[...]


def split_pairs(pairs_ref, wide_ref, even_ref, odd_ref, rows):
    def body(i, carry):
        start = pl.multiple_of(i * rows, rows)
        wide_ref[...] = pairs_ref[pl.ds(pl.multiple_of(i * 2 * rows, 2 * rows), 2 * rows), :].astype(
            jnp.float32
        )
        even_ref[pl.ds(start, rows), :] = wide_ref[pl.ds(0, rows, stride=2), :].astype(jnp.bfloat16)
        odd_ref[pl.ds(start, rows), :] = wide_ref[pl.ds(1, rows, stride=2), :].astype(jnp.bfloat16)
        return carry

    lax.fori_loop(0, even_ref.shape[0] // rows, body, 0)


def segment_normalize(tensor):
    values = tensor.astype(jnp.float32)
    squares = values * values
    head_of = lax.broadcasted_iota(jnp.int32, values.shape, 1) // HEAD_DIM
    scale = jnp.zeros_like(values)
    for head in range(values.shape[1] // HEAD_DIM):
        mine = head_of == head
        mean = jnp.sum(jnp.where(mine, squares, 0.0), axis=-1, keepdims=True) / HEAD_DIM
        scale = jnp.where(mine, lax.rsqrt(mean + epsilon), scale)
    return values * scale


def attend(queries, keys, values):
    query_hat = segment_normalize(queries)
    key_hat = segment_normalize(keys).astype(jnp.bfloat16)
    head_of = lax.broadcasted_iota(jnp.int32, query_hat.shape, 1) // HEAD_DIM
    mixed = jnp.zeros(query_hat.shape, jnp.float32)
    for head in range(query_hat.shape[1] // HEAD_DIM):
        mine = head_of == head
        own = jnp.where(mine, query_hat, 0.0).astype(jnp.bfloat16)
        scores = lax.dot_general(
            own, key_hat, (((1,), (1,)), ((), ())), preferred_element_type=jnp.float32
        ) * HEAD_DIM ** (-0.5)
        weights = softmax_weights(scores)
        mixed = jnp.where(mine, jnp.dot(weights, values, preferred_element_type=jnp.float32), mixed)
    return mixed.astype(jnp.bfloat16)


def modulate_rows(states, modulation_ref, first):
    normed = states * lax.rsqrt(jnp.mean(states * states, axis=-1, keepdims=True) + epsilon)
    return (
        normed * (1.0 + modulation_ref[first + 1 : first + 2, :]) + modulation_ref[first : first + 1, :]
    ).astype(jnp.bfloat16)


def project(rows_ref, weight_ref):
    return jnp.dot(rows_ref[...], weight_ref[...], preferred_element_type=jnp.float32).astype(jnp.bfloat16)


def block_kernel(count, video_width, audio_width, *refs):
    video_state, audio_state, video_mod, audio_mod = refs[:4]
    weights_hbm = refs[4:14]
    video_out, audio_out = refs[14:16]
    weights = refs[16:26]
    rest = refs[26:]
    size = 13
    video1, audio1, video2, audio2 = (
        Stream(rest[i * size : (i + 1) * size], count) for i in range(4)
    )
    (weight_sem, pair_wide, video_key, video_value, audio_key, audio_value,
     video_mixed, audio_mixed, video_hidden, audio_hidden) = rest[4 * size :]
    loads = [
        pltpu.make_async_copy(hbm, vmem, weight_sem.at[i])
        for i, (hbm, vmem) in enumerate(zip(weights_hbm, weights))
    ]
    (audio_query, audio_pairs, video_query, video_pairs, audio_output, video_output,
     audio_expand, audio_shrink, video_expand, video_shrink) = weights
    for load in loads:
        load.start()

    barrier = pltpu.get_barrier_semaphore()
    for step in range(1, video1.chips):
        pl.semaphore_signal(
            barrier,
            inc=1,
            device_id={"tensor": video1.distant(step) * 2 + video1.core},
            device_id_type=pl.DeviceIdType.MESH,
        )
    pl.semaphore_signal(
        barrier, inc=1, device_id={"tensor": video1.mate}, device_id_type=pl.DeviceIdType.MESH
    )
    audio1.own[...] = modulate_rows(audio_state[...], audio_mod, 0)
    video1.own[...] = modulate_rows(video_state[...], video_mod, 0)
    pl.semaphore_wait(barrier, video1.chips)

    audio1.gather_start()
    video1.gather_start()
    loads[1].wait()
    split_pairs(audio_pairs, pair_wide, audio_key, audio_value, pair_wide.shape[0] // 2)
    audio1.gather_forward()
    loads[3].wait()
    split_pairs(video_pairs, pair_wide, video_key, video_value, pair_wide.shape[0] // 2)
    audio1.gather_finish()
    loads[0].wait()
    audio_queries = project(audio1.whole, audio_query)
    audio_keys = project(audio1.whole, audio_key)
    audio_values = project(audio1.whole, audio_value)
    video1.gather_forward()
    video1.gather_finish()
    loads[2].wait()
    video_keys = project(video1.whole, video_key)
    video_values = project(video1.whole, video_value)
    audio_mixed[...] = attend(audio_queries, video_keys, video_values)
    loads[4].wait()
    matmul_to(audio_mixed, audio_output, 512, audio1.emit)
    audio1.scatter_start()
    video_queries = project(video1.whole, video_query)
    video_mixed[...] = attend(video_queries, audio_keys, audio_values)
    audio1.scatter_send_on()
    loads[5].wait()
    matmul_to(video_mixed, video_output, 512, video1.emit)
    video1.scatter_start()
    audio1.gather_drain()
    video1.gather_drain()
    video1.scatter_send_on()
    audio_mid = audio_state[...] + audio_mod[2:3, :] * audio1.scatter_finish()
    audio_out[...] = audio_mid
    audio2.own[...] = modulate_rows(audio_mid, audio_mod, 3)
    audio2.gather_start()
    video_mid = video_state[...] + video_mod[2:3, :] * video1.scatter_finish()
    video_out[...] = video_mid
    video2.own[...] = modulate_rows(video_mid, video_mod, 3)
    video2.gather_start()
    audio2.gather_forward()
    audio2.gather_finish()

    def keep_hidden(target):
        def emit(columns, product):
            target[:, columns] = jax.nn.gelu(product, approximate=True).astype(jnp.bfloat16)

        return emit

    loads[6].wait()
    matmul_to(audio2.whole, audio_expand, 256, keep_hidden(audio_hidden))
    loads[7].wait()
    matmul_to(audio_hidden, audio_shrink, 512, audio2.emit)
    audio2.scatter_start()
    video2.gather_forward()
    audio2.scatter_send_on()
    video2.gather_finish()
    loads[8].wait()
    matmul_to(video2.whole, video_expand, 256, keep_hidden(video_hidden))
    loads[9].wait()
    matmul_to(video_hidden, video_shrink, 512, video2.emit)
    video2.scatter_start()
    audio_out[...] += audio_mod[5:6, :] * audio2.scatter_finish()
    audio2.gather_drain()
    video2.gather_drain()
    video2.scatter_send_on()
    video_out[...] += video_mod[5:6, :] * video2.scatter_finish()


def fused_block(
    video_state,
    audio_state,
    video_modulation,
    audio_modulation,
    video_query,
    audio_keyval,
    video_output,
    audio_query,
    video_keyval,
    audio_output,
    video_expand,
    video_shrink,
    audio_expand,
    audio_shrink,
):
    count = lax.axis_size("tensor")
    rows, video_width = video_state.shape
    audio_width = audio_state.shape[1]
    width = video_query.shape[1]
    tokens = count * rows
    weights = (
        audio_query,
        audio_keyval.reshape(-1, width),
        video_query,
        video_keyval.reshape(-1, width),
        audio_output,
        video_output,
        audio_expand,
        audio_shrink,
        video_expand,
        video_shrink,
    )
    vmem = pl.BlockSpec(memory_space=pltpu.VMEM)
    hbm = pl.BlockSpec(memory_space=pl.ANY)
    streams = []
    for extent in (video_width, audio_width) * 2:
        streams += Stream.scratch(count, rows, extent)
    bf16 = jnp.bfloat16
    return pl.pallas_call(
        functools.partial(block_kernel, count, video_width, audio_width),
        out_shape=(
            jax.ShapeDtypeStruct(video_state.shape, jnp.float32),
            jax.ShapeDtypeStruct(audio_state.shape, jnp.float32),
        ),
        in_specs=[vmem] * 4 + [hbm] * len(weights),
        out_specs=(vmem, vmem),
        scratch_shapes=[pltpu.VMEM(weight.shape, weight.dtype) for weight in weights]
        + streams
        + [
            pltpu.SemaphoreType.DMA((len(weights),)),
            pltpu.VMEM((512, width), jnp.float32),
            pltpu.VMEM((video_width, width), bf16),
            pltpu.VMEM((video_width, width), bf16),
            pltpu.VMEM((audio_width, width), bf16),
            pltpu.VMEM((audio_width, width), bf16),
            pltpu.VMEM((tokens, width), bf16),
            pltpu.VMEM((tokens, width), bf16),
            pltpu.VMEM((tokens, video_expand.shape[1]), bf16),
            pltpu.VMEM((tokens, audio_expand.shape[1]), bf16),
        ],
        compiler_params=pltpu.CompilerParams(
            collective_id=0, has_side_effects=True, vmem_limit_bytes=VMEM_BYTES
        ),
    )(video_state, audio_state, video_modulation, audio_modulation, *weights)


def block(*arrays):
    count = lax.axis_size("tensor")
    rows = arrays[0].shape[0]
    width = arrays[4].shape[1]
    held = sum(array.size * array.dtype.itemsize for array in arrays[4:])
    fits = held <= WEIGHT_BYTES and count * rows <= 64
    shaped = count % 2 == 0 and 2 * rows % 8 == 0 and width % 128 == 0
    tiled = all(extent % 512 == 0 for array in (arrays[0], arrays[1], arrays[10], arrays[12]) for extent in array.shape[1:])
    return fused_block(*arrays) if fits and shaped and tiled else on_device(*arrays)


def solution(mesh):
    placed = (
        P(("groups", "tensor"), None),
        P(("groups", "tensor"), None),
        P("groups", None),
        P("groups", None),
        P(None, "tensor"),
        P(None, None, "tensor"),
        P("tensor", None),
        P(None, "tensor"),
        P(None, None, "tensor"),
        P("tensor", None),
        P(None, "tensor"),
        P("tensor", None),
        P(None, "tensor"),
        P("tensor", None),
    )
    return jax.shard_map(
        block,
        mesh=mesh,
        in_specs=placed,
        out_specs=(P(("groups", "tensor"), None), P(("groups", "tensor"), None)),
        check_vma=False,
    )
```

```python
import functools

import jax
import jax.numpy as jnp
from jax import lax
from jax.experimental import pallas as pl
from jax.experimental.pallas import tpu as pltpu
from jax.sharding import PartitionSpec as P

HEAD_DIM = 64


epsilon = 1e-06


def partner(block, axis, distance):
    count = lax.axis_size(axis)
    route = []
    for low in range(count):
        high = low | 1 << distance
        if high != low and high < count:
            route += [(low, high), (high, low)]
    return lax.ppermute(block, axis, route)


def modulate(states, modulation, first):
    normed = states * lax.rsqrt(jnp.mean(states * states, axis=-1, keepdims=True) + epsilon)
    return (normed * (1.0 + modulation[first + 1]) + modulation[first]).astype(jnp.bfloat16)


def head_normalize(tensor):
    values = tensor.astype(jnp.float32)
    return (values * lax.rsqrt(jnp.mean(values * values, axis=-1, keepdims=True) + epsilon)).astype(
        jnp.bfloat16
    )


def softmax_weights(scores):
    expo = jnp.exp(scores)
    return (expo / jnp.sum(expo, axis=-1, keepdims=True)).astype(jnp.bfloat16)


def local_heads(queries, key_part, value_part):
    query_count, width = queries.shape
    source_count = key_part.shape[0]
    head_count = width // HEAD_DIM
    query_hat = head_normalize(queries.reshape(query_count, head_count, HEAD_DIM))
    key_hat = head_normalize(key_part.reshape(source_count, head_count, HEAD_DIM))
    scores = jnp.einsum(
        "qhd,khd->hqk", query_hat, key_hat, preferred_element_type=jnp.float32
    ) * HEAD_DIM ** (-0.5)
    weights = softmax_weights(scores)
    values = value_part.reshape(source_count, head_count, HEAD_DIM)
    mixed = jnp.einsum("hqk,khd->qhd", weights, values, preferred_element_type=jnp.float32)
    return mixed.astype(jnp.bfloat16).reshape(query_count, width)


def project_attend(query_rows, source_rows, query_weight, keyval_weight):
    width = query_weight.shape[1]
    queries = jnp.dot(query_rows, query_weight, preferred_element_type=jnp.float32).astype(
        jnp.bfloat16
    )
    flat_weight = keyval_weight.reshape(keyval_weight.shape[0], 2 * width)
    keyvals = jnp.dot(source_rows, flat_weight, preferred_element_type=jnp.float32).astype(
        jnp.bfloat16
    )
    key_part = keyvals[:, :width]
    value_part = keyvals[:, width:]
    if width >= HEAD_DIM:
        return local_heads(queries, key_part, value_part)
    query_float = queries.astype(jnp.float32)
    key_float = key_part.astype(jnp.float32)
    query_square = jnp.sum(query_float * query_float, axis=1, keepdims=True)
    key_square = jnp.sum(key_float * key_float, axis=1, keepdims=True)
    other_query, other_key = partner((query_square, key_square), "tensor", 0)
    query_hat = (query_float * lax.rsqrt((query_square + other_query) / HEAD_DIM + epsilon)).astype(
        jnp.bfloat16
    )
    key_hat = (key_float * lax.rsqrt((key_square + other_key) / HEAD_DIM + epsilon)).astype(
        jnp.bfloat16
    )
    partial_scores = jnp.einsum("qd,kd->qk", query_hat, key_hat, preferred_element_type=jnp.float32)
    other_scores = partner(partial_scores, "tensor", 0)
    scores = (partial_scores + other_scores) * HEAD_DIM ** (-0.5)
    weights = softmax_weights(scores)
    return jnp.dot(weights, value_part, preferred_element_type=jnp.float32).astype(jnp.bfloat16)


def output_rows(mixed, weight):
    return jnp.dot(mixed, weight, preferred_element_type=jnp.float32)


def feed_rows(inputs, expand, shrink):
    hidden = jnp.dot(inputs, expand, preferred_element_type=jnp.float32)
    hidden = jax.nn.gelu(hidden, approximate=True).astype(jnp.bfloat16)
    return jnp.dot(hidden, shrink, preferred_element_type=jnp.float32)


def on_device(
    video_state,
    audio_state,
    video_modulation,
    audio_modulation,
    video_query,
    audio_keyval,
    video_output,
    audio_query,
    video_keyval,
    audio_output,
    video_expand,
    video_shrink,
    audio_expand,
    audio_shrink,
):
    video_count = video_state.shape[0]
    audio_own = modulate(audio_state, audio_modulation, 0)
    video_whole = lax.all_gather(video_state, "tensor", axis=0, tiled=True)
    video_normed = modulate(video_whole, video_modulation, 0)
    audio_normed = lax.all_gather(audio_own, "tensor", axis=0, tiled=True)
    video_mixed = project_attend(video_normed, audio_normed, video_query, audio_keyval)
    audio_mixed = project_attend(audio_normed, video_normed, audio_query, video_keyval)
    audio_term = lax.psum_scatter(
        output_rows(audio_mixed, audio_output), "tensor", scatter_dimension=0, tiled=True
    )
    audio_mid = audio_state + audio_modulation[2] * audio_term
    audio_inner_own = modulate(audio_mid, audio_modulation, 3)
    partial_term = jnp.dot(video_mixed, video_output, preferred_element_type=jnp.float32)
    full_term = lax.psum(partial_term, "tensor")
    video_mid_whole = video_whole + video_modulation[2] * full_term
    video_inner = modulate(video_mid_whole, video_modulation, 3)
    first_row = lax.axis_index("tensor") * video_count
    video_mid = lax.dynamic_slice_in_dim(video_mid_whole, first_row, video_count, 0)
    audio_inner = lax.all_gather(audio_inner_own, "tensor", axis=0, tiled=True)
    video_feed = lax.psum_scatter(
        feed_rows(video_inner, video_expand, video_shrink),
        "tensor",
        scatter_dimension=0,
        tiled=True,
    )
    audio_feed = lax.psum_scatter(
        feed_rows(audio_inner, audio_expand, audio_shrink),
        "tensor",
        scatter_dimension=0,
        tiled=True,
    )
    video_next = video_mid + video_modulation[5] * video_feed
    audio_next = audio_mid + audio_modulation[5] * audio_feed
    return (video_next, audio_next)


VMEM_BYTES = 66_000_000
WEIGHT_BYTES = 40 << 20


def matmul_to(lhs_ref, weight_ref, first, extent, tile, emit):
    def body(i, carry):
        start = pl.multiple_of(i * tile, tile)
        columns = pl.ds(pl.multiple_of(first + i * tile, tile), tile)
        emit(start, jnp.dot(lhs_ref[...], weight_ref[:, columns], preferred_element_type=jnp.float32))
        return carry

    lax.fori_loop(0, extent // tile, body, 0)


class Stream:
    names = ("own", "slots", "wide", "other", "paired", "across", "crossed", "sums", "terms", "total")

    @staticmethod
    def scratch(count, rows, width):
        chips, planes = count // 2, count // 4
        return [
            pltpu.VMEM((rows, width), jnp.bfloat16),
            pltpu.VMEM((count, rows, width), jnp.bfloat16),
            pltpu.VMEM((chips, 2 * rows, width), jnp.float32),
            pltpu.VMEM((chips, rows, width), jnp.bfloat16),
            pltpu.VMEM((chips, rows, width), jnp.bfloat16),
            pltpu.VMEM((planes, rows, width), jnp.bfloat16),
            pltpu.VMEM((planes, rows, width), jnp.bfloat16),
            pltpu.VMEM((planes, rows, width), jnp.bfloat16),
            pltpu.VMEM((planes, rows, width), jnp.bfloat16),
            pltpu.VMEM((rows, width), jnp.float32),
            pltpu.SemaphoreType.DMA((chips,)),
            pltpu.SemaphoreType.DMA((planes,)),
            pltpu.SemaphoreType.DMA((planes,)),
            pltpu.SemaphoreType.DMA((count,)),
            pltpu.SemaphoreType.DMA((planes + 2,)),
            pltpu.SemaphoreType.DMA((planes + 2,)),
        ]

    def __init__(self, refs, whole, count):
        for name, ref in zip(self.names, refs):
            setattr(self, name, ref)
        (self.mate_send, self.side_send, self.plane_send, self.gather_recv, self.scatter_send,
         self.scatter_recv) = refs[len(self.names):]
        self.whole = whole
        self.count, self.chips, self.planes = count, count // 2, count // 4
        self.rows = self.own.shape[0]
        self.me = lax.axis_index("tensor")
        self.core, self.chip = self.me % 2, self.me // 2
        self.side, self.plane = self.chip % 2, self.chip // 2
        self.mate = self.at(self.plane, self.side, 1 - self.core)
        self.beside = self.at(self.plane, 1 - self.side, self.core)

    @staticmethod
    def at(plane, side, core):
        return (plane * 2 + side) * 2 + core

    def distant(self, step):
        return lax.rem(self.plane + step, self.planes)

    def send(self, slot, source, semaphore, goal):
        return pltpu.make_async_remote_copy(
            src_ref=source,
            dst_ref=self.slots.at[slot],
            send_sem=semaphore,
            recv_sem=self.gather_recv.at[slot],
            device_id={"tensor": goal},
            device_id_type=pl.DeviceIdType.MESH,
        )

    def to_plane(self, step):
        goal = self.at(self.distant(step), self.side, self.core)
        return self.send(self.me, self.own, self.plane_send.at[step], goal)

    def to_side(self, step):
        slot = self.at(self.distant(step), self.side, self.core)
        source = self.slots.at[slot] if step else self.own
        return self.send(slot, source, self.side_send.at[step], self.beside)

    def to_mate(self, step, side):
        slot = self.at(self.distant(step), self.side if side == 0 else 1 - self.side, self.core)
        source = self.slots.at[slot] if step or side else self.own
        return self.send(slot, source, self.mate_send.at[2 * step + side], self.mate)

    def keep(self):
        return pltpu.make_async_copy(self.own, self.slots.at[self.me], self.gather_recv.at[self.me])

    def arrived(self, slot):
        pltpu.make_async_copy(self.slots.at[slot], self.slots.at[slot], self.gather_recv.at[slot]).wait()

    def gather_start(self):
        for step in range(1, self.planes):
            self.to_plane(step).start()
        self.to_side(0).start()
        self.to_mate(0, 0).start()
        self.keep().start()

    def gather_planes(self):
        for step in range(1, self.planes):
            self.arrived(self.at(self.distant(step), self.side, self.core))
            self.to_side(step).start()
            self.to_mate(step, 0).start()

    def gather_sides(self):
        for step in range(self.planes):
            self.arrived(self.at(self.distant(step), 1 - self.side, self.core))
            self.to_mate(step, 1).start()

    def gather_finish(self):
        self.keep().wait()
        for step in range(self.planes):
            for side in range(2):
                self.arrived(self.at(self.distant(step), side, 1 - self.core))

        def widen(chip, carry):
            self.wide[chip, : self.rows, :] = self.slots[2 * chip].astype(jnp.float32)
            self.wide[chip, self.rows :, :] = self.slots[2 * chip + 1].astype(jnp.float32)
            return carry

        lax.fori_loop(0, self.chips, widen, 0)
        self.whole[...] = self.wide[...].reshape(self.whole.shape).astype(jnp.bfloat16)

    def gather_drain(self):
        for step in range(self.planes):
            if step:
                self.to_plane(step).wait_send()
            self.to_side(step).wait_send()
            for side in range(2):
                self.to_mate(step, side).wait_send()

    def emit(self, offset=0):
        def keep(start, product):
            columns = pl.ds(pl.multiple_of(start + offset, 128), product.shape[1])
            self.wide[:, :, columns] = product.reshape(self.chips, 2 * self.rows, product.shape[1])

        return keep

    def trade(self, source, target, index, goal):
        return pltpu.make_async_remote_copy(
            src_ref=source,
            dst_ref=target,
            send_sem=self.scatter_send.at[index],
            recv_sem=self.scatter_recv.at[index],
            device_id={"tensor": goal},
            device_id_type=pl.DeviceIdType.MESH,
        )

    def swap(self):
        return self.trade(self.other, self.paired, self.planes, self.mate)

    def cross(self):
        return self.trade(self.across, self.crossed, self.planes + 1, self.beside)

    def halves(self, chip):
        rows = self.wide[chip]
        low, high = rows[: self.rows], rows[self.rows :]
        first = self.core == 0
        return jnp.where(first, low, high), jnp.where(first, high, low)

    def of_pair(self, plane, side):
        chip = plane * 2 + side
        return self.halves(chip)[0] + self.paired[chip].astype(jnp.float32)

    def scatter_start(self):
        def body(chip, carry):
            self.other[chip] = self.halves(chip)[1].astype(jnp.bfloat16)
            return carry

        lax.fori_loop(0, self.chips, body, 0)
        self.swap().start()

    def scatter_sides(self):
        self.swap().wait()

        def body(plane, carry):
            self.across[plane] = self.of_pair(plane, 1 - self.side).astype(jnp.bfloat16)
            return carry

        lax.fori_loop(0, self.planes, body, 0)
        self.cross().start()

    def of_column(self, plane):
        return self.of_pair(plane, self.side) + self.crossed[plane].astype(jnp.float32)

    def term(self, step):
        goal = self.distant(step)
        return pltpu.make_async_remote_copy(
            src_ref=self.sums.at[goal],
            dst_ref=self.terms.at[self.plane],
            send_sem=self.scatter_send.at[step],
            recv_sem=self.scatter_recv.at[self.plane],
            device_id={"tensor": self.at(goal, self.side, self.core)},
            device_id_type=pl.DeviceIdType.MESH,
        )

    def scatter_planes(self):
        self.cross().wait()
        for step in range(1, self.planes):
            goal = self.distant(step)
            self.sums[goal] = self.of_column(goal).astype(jnp.bfloat16)
            self.term(step).start()
        self.total[...] = self.of_column(self.plane)

    def scatter_finish(self):
        result = self.total[...]
        for step in range(1, self.planes):
            source = self.distant(step)
            pltpu.make_async_copy(
                self.terms.at[source], self.terms.at[source], self.scatter_recv.at[source]
            ).wait()
            result += self.terms[source].astype(jnp.float32)
        for step in range(1, self.planes):
            self.term(step).wait_send()
        return result


def split_pairs(pairs_ref, wide_ref, even_ref, odd_ref, rows):
    def body(i, carry):
        start = pl.multiple_of(i * rows, rows)
        wide_ref[...] = pairs_ref[pl.ds(pl.multiple_of(i * 2 * rows, 2 * rows), 2 * rows), :].astype(
            jnp.float32
        )
        even_ref[pl.ds(start, rows), :] = wide_ref[pl.ds(0, rows, stride=2), :].astype(jnp.bfloat16)
        odd_ref[pl.ds(start, rows), :] = wide_ref[pl.ds(1, rows, stride=2), :].astype(jnp.bfloat16)
        return carry

    lax.fori_loop(0, even_ref.shape[0] // rows, body, 0)


def segment_normalize(tensor):
    values = tensor.astype(jnp.float32)
    squares = values * values
    head_of = lax.broadcasted_iota(jnp.int32, values.shape, 1) // HEAD_DIM
    scale = jnp.zeros_like(values)
    for head in range(values.shape[1] // HEAD_DIM):
        mine = head_of == head
        mean = jnp.sum(jnp.where(mine, squares, 0.0), axis=-1, keepdims=True) / HEAD_DIM
        scale = jnp.where(mine, lax.rsqrt(mean + epsilon), scale)
    return values * scale


def attend(queries, keys, values):
    query_hat = segment_normalize(queries)
    key_hat = segment_normalize(keys).astype(jnp.bfloat16)
    head_of = lax.broadcasted_iota(jnp.int32, query_hat.shape, 1) // HEAD_DIM
    mixed = jnp.zeros(query_hat.shape, jnp.float32)
    for head in range(query_hat.shape[1] // HEAD_DIM):
        mine = head_of == head
        own = jnp.where(mine, query_hat, 0.0).astype(jnp.bfloat16)
        scores = lax.dot_general(
            own, key_hat, (((1,), (1,)), ((), ())), preferred_element_type=jnp.float32
        ) * HEAD_DIM ** (-0.5)
        weights = softmax_weights(scores)
        mixed = jnp.where(mine, jnp.dot(weights, values, preferred_element_type=jnp.float32), mixed)
    return mixed.astype(jnp.bfloat16)


def modulate_rows(states, modulation_ref, first):
    normed = states * lax.rsqrt(jnp.mean(states * states, axis=-1, keepdims=True) + epsilon)
    return (
        normed * (1.0 + modulation_ref[first + 1 : first + 2, :]) + modulation_ref[first : first + 1, :]
    ).astype(jnp.bfloat16)


def project(rows, weight):
    return jnp.dot(rows, weight, preferred_element_type=jnp.float32)


def block_kernel(count, *refs):
    video_state, audio_state, video_mod, audio_mod = refs[:4]
    weights_hbm = refs[4:14]
    video_out, audio_out = refs[14:16]
    weights = refs[16:26]
    (weight_sem, pair_wide, video_key, video_value, audio_key, audio_value, video_mixed, audio_mixed,
     video_hidden, audio_hidden, video_sums, video_whole, audio_whole) = refs[26:39]
    rest = refs[39:]
    size = len(rest) // 6
    half = video_state.shape[1] // 2
    wholes = (audio_whole, video_whole.at[:, :half], video_whole.at[:, half:]) * 2
    audio1, left1, right1, audio2, left2, right2 = (
        Stream(rest[i * size : (i + 1) * size], wholes[i], count) for i in range(6)
    )
    loads = [
        pltpu.make_async_copy(hbm, vmem, weight_sem.at[i])
        for i, (hbm, vmem) in enumerate(zip(weights_hbm, weights))
    ]
    (audio_query, audio_pairs, video_query, video_pairs, audio_output, video_output,
     audio_expand, audio_shrink, video_expand, video_shrink) = weights
    for load in loads:
        load.start()

    barrier = pltpu.get_barrier_semaphore()
    friends = [audio1.at(audio1.distant(step), audio1.side, audio1.core) for step in range(1, audio1.planes)]
    friends += [audio1.mate, audio1.beside]
    for friend in friends:
        pl.semaphore_signal(
            barrier, inc=1, device_id={"tensor": friend}, device_id_type=pl.DeviceIdType.MESH
        )
    audio1.own[...] = modulate_rows(audio_state[...], audio_mod, 0)
    video_own = modulate_rows(video_state[...], video_mod, 0)
    left1.own[...] = video_own[:, :half]
    right1.own[...] = video_own[:, half:]
    pl.semaphore_wait(barrier, len(friends))

    audio1.gather_start()
    left1.gather_start()
    right1.gather_start()
    loads[1].wait()
    split_pairs(audio_pairs, pair_wide, audio_key, audio_value, pair_wide.shape[0] // 2)
    audio1.gather_planes()
    loads[3].wait()
    split_pairs(video_pairs, pair_wide, video_key, video_value, pair_wide.shape[0] // 2)
    audio1.gather_sides()
    left1.gather_planes()
    audio1.gather_finish()
    loads[0].wait()
    bf16 = jnp.bfloat16
    audio_queries = project(audio_whole[...], audio_query[...]).astype(bf16)
    left1.gather_sides()
    right1.gather_planes()
    audio_keys = project(audio_whole[...], audio_key[...]).astype(bf16)
    audio_values = project(audio_whole[...], audio_value[...]).astype(bf16)
    left1.gather_finish()
    loads[2].wait()
    rows = left1.whole[...]
    video_keys = project(rows, video_key[:half, :])
    right1.gather_sides()
    video_values = project(rows, video_value[:half, :])
    video_queries = project(rows, video_query[:half, :])
    right1.gather_finish()
    rows = right1.whole[...]
    video_keys = (video_keys + project(rows, video_key[half:, :])).astype(bf16)
    video_values = (video_values + project(rows, video_value[half:, :])).astype(bf16)
    video_queries = (video_queries + project(rows, video_query[half:, :])).astype(bf16)
    video_mixed[...] = attend(video_queries, audio_keys, audio_values)
    loads[5].wait()
    matmul_to(video_mixed, video_output, 0, half, 512, left1.emit())
    left1.scatter_start()
    matmul_to(video_mixed, video_output, half, half, 512, right1.emit())
    right1.scatter_start()
    left1.scatter_sides()
    audio_mixed[...] = attend(audio_queries, video_keys, video_values)
    right1.scatter_sides()
    loads[4].wait()
    matmul_to(audio_mixed, audio_output, 0, audio_output.shape[1], 512, audio1.emit())
    audio1.scatter_start()
    left1.scatter_planes()
    audio1.scatter_sides()
    right1.scatter_planes()
    audio1.gather_drain()
    left1.gather_drain()
    right1.gather_drain()
    audio1.scatter_planes()
    video_mid = video_state[...] + video_mod[2:3, :] * jnp.concatenate(
        [left1.scatter_finish(), right1.scatter_finish()], axis=1
    )
    video_out[...] = video_mid
    video_own = modulate_rows(video_mid, video_mod, 3)
    left2.own[...] = video_own[:, :half]
    right2.own[...] = video_own[:, half:]
    left2.gather_start()
    right2.gather_start()
    audio_mid = audio_state[...] + audio_mod[2:3, :] * audio1.scatter_finish()
    audio_out[...] = audio_mid
    audio2.own[...] = modulate_rows(audio_mid, audio_mod, 3)
    audio2.gather_start()
    left2.gather_planes()
    right2.gather_planes()
    left2.gather_sides()
    audio2.gather_planes()
    left2.gather_finish()
    loads[8].wait()
    hidden_width = video_hidden.shape[1]

    def keep_sums(start, product):
        video_sums[:, pl.ds(start, product.shape[1])] = product

    def keep_video(start, product):
        columns = pl.ds(start, product.shape[1])
        video_hidden[:, columns] = jax.nn.gelu(video_sums[:, columns] + product, approximate=True).astype(bf16)

    def keep_audio(start, product):
        audio_hidden[:, pl.ds(start, product.shape[1])] = jax.nn.gelu(product, approximate=True).astype(bf16)

    right2.gather_sides()
    matmul_to(left2.whole, video_expand.at[:half, :], 0, hidden_width, 256, keep_sums)
    audio2.gather_sides()
    right2.gather_finish()
    matmul_to(right2.whole, video_expand.at[half:, :], 0, hidden_width, 256, keep_video)
    loads[9].wait()
    matmul_to(video_hidden, video_shrink, 0, half, 512, left2.emit())
    left2.scatter_start()
    matmul_to(video_hidden, video_shrink, half, half, 512, right2.emit())
    right2.scatter_start()
    left2.scatter_sides()
    audio2.gather_finish()
    loads[6].wait()
    matmul_to(audio2.whole, audio_expand, 0, audio_hidden.shape[1], 256, keep_audio)
    right2.scatter_sides()
    loads[7].wait()
    matmul_to(audio_hidden, audio_shrink, 0, audio_shrink.shape[1], 512, audio2.emit())
    audio2.scatter_start()
    left2.scatter_planes()
    audio2.scatter_sides()
    right2.scatter_planes()
    audio2.gather_drain()
    left2.gather_drain()
    right2.gather_drain()
    audio2.scatter_planes()
    video_out[:, :half] += video_mod[5:6, :half] * left2.scatter_finish()
    video_out[:, half:] += video_mod[5:6, half:] * right2.scatter_finish()
    audio_out[...] += audio_mod[5:6, :] * audio2.scatter_finish()


def hand_over(video_ref, audio_ref, video_out, audio_out):
    video_out[...] = video_ref[...]
    audio_out[...] = audio_ref[...]


def fused_block(
    video_state,
    audio_state,
    video_modulation,
    audio_modulation,
    video_query,
    audio_keyval,
    video_output,
    audio_query,
    video_keyval,
    audio_output,
    video_expand,
    video_shrink,
    audio_expand,
    audio_shrink,
):
    count = lax.axis_size("tensor")
    rows, video_width = video_state.shape
    audio_width = audio_state.shape[1]
    width = video_query.shape[1]
    tokens = count * rows
    weights = (
        audio_query,
        audio_keyval.reshape(-1, width),
        video_query,
        video_keyval.reshape(-1, width),
        audio_output,
        video_output,
        audio_expand,
        audio_shrink,
        video_expand,
        video_shrink,
    )
    vmem = pl.BlockSpec(memory_space=pltpu.VMEM)
    hbm = pl.BlockSpec(memory_space=pl.ANY)
    streams = []
    for extent in (audio_width, video_width // 2, video_width // 2) * 2:
        streams += Stream.scratch(count, rows, extent)
    bf16 = jnp.bfloat16
    results = (
        jax.ShapeDtypeStruct(video_state.shape, jnp.float32),
        jax.ShapeDtypeStruct(audio_state.shape, jnp.float32),
    )
    video_next, audio_next = pl.pallas_call(
        functools.partial(block_kernel, count),
        out_shape=results,
        in_specs=[vmem] * 4 + [hbm] * len(weights),
        out_specs=(vmem, vmem),
        scratch_shapes=[pltpu.VMEM(weight.shape, weight.dtype) for weight in weights]
        + [
            pltpu.SemaphoreType.DMA((len(weights),)),
            pltpu.VMEM((512, width), jnp.float32),
            pltpu.VMEM((video_width, width), bf16),
            pltpu.VMEM((video_width, width), bf16),
            pltpu.VMEM((audio_width, width), bf16),
            pltpu.VMEM((audio_width, width), bf16),
            pltpu.VMEM((tokens, width), bf16),
            pltpu.VMEM((tokens, width), bf16),
            pltpu.VMEM((tokens, video_expand.shape[1]), bf16),
            pltpu.VMEM((tokens, audio_expand.shape[1]), bf16),
            pltpu.VMEM((tokens, video_expand.shape[1]), jnp.float32),
            pltpu.VMEM((tokens, video_width), bf16),
            pltpu.VMEM((tokens, audio_width), bf16),
        ]
        + streams,
        compiler_params=pltpu.CompilerParams(
            collective_id=0, has_side_effects=True, vmem_limit_bytes=VMEM_BYTES
        ),
    )(video_state, audio_state, video_modulation, audio_modulation, *weights)
    return pl.pallas_call(
        hand_over, out_shape=results, in_specs=[vmem] * 2, out_specs=(vmem, vmem)
    )(video_next, audio_next)


def block(*arrays):
    count = lax.axis_size("tensor")
    rows = arrays[0].shape[0]
    width = arrays[4].shape[1]
    held = sum(array.size * array.dtype.itemsize for array in arrays[4:])
    fits = held <= WEIGHT_BYTES and count * rows <= 64
    shaped = count % 4 == 0 and 2 * rows % 8 == 0 and width % 128 == 0
    tiled = all(array.shape[1] % 1024 == 0 for array in arrays[:2]) and all(
        arrays[i].shape[1] % 256 == 0 for i in (10, 12)
    )
    return fused_block(*arrays) if fits and shaped and tiled else on_device(*arrays)


def solution(mesh):
    placed = (
        P(("groups", "tensor"), None),
        P(("groups", "tensor"), None),
        P("groups", None),
        P("groups", None),
        P(None, "tensor"),
        P(None, None, "tensor"),
        P("tensor", None),
        P(None, "tensor"),
        P(None, None, "tensor"),
        P("tensor", None),
        P(None, "tensor"),
        P("tensor", None),
        P(None, "tensor"),
        P("tensor", None),
    )
    return jax.shard_map(
        block,
        mesh=mesh,
        in_specs=placed,
        out_specs=(P(("groups", "tensor"), None), P(("groups", "tensor"), None)),
        check_vma=False,
    )
```

```python
import functools

import jax
import jax.numpy as jnp
from jax import lax
from jax.experimental import pallas as pl
from jax.experimental.pallas import tpu as pltpu
from jax.sharding import PartitionSpec as P

HEAD_DIM = 64


epsilon = 1e-06


def partner(block, axis, distance):
    count = lax.axis_size(axis)
    route = []
    for low in range(count):
        high = low | 1 << distance
        if high != low and high < count:
            route += [(low, high), (high, low)]
    return lax.ppermute(block, axis, route)


def modulate(states, modulation, first):
    normed = states * lax.rsqrt(jnp.mean(states * states, axis=-1, keepdims=True) + epsilon)
    return (normed * (1.0 + modulation[first + 1]) + modulation[first]).astype(jnp.bfloat16)


def head_normalize(tensor):
    values = tensor.astype(jnp.float32)
    return (values * lax.rsqrt(jnp.mean(values * values, axis=-1, keepdims=True) + epsilon)).astype(
        jnp.bfloat16
    )


def softmax_weights(scores):
    expo = jnp.exp(scores)
    return (expo / jnp.sum(expo, axis=-1, keepdims=True)).astype(jnp.bfloat16)


def local_heads(queries, key_part, value_part):
    query_count, width = queries.shape
    source_count = key_part.shape[0]
    head_count = width // HEAD_DIM
    query_hat = head_normalize(queries.reshape(query_count, head_count, HEAD_DIM))
    key_hat = head_normalize(key_part.reshape(source_count, head_count, HEAD_DIM))
    scores = jnp.einsum(
        "qhd,khd->hqk", query_hat, key_hat, preferred_element_type=jnp.float32
    ) * HEAD_DIM ** (-0.5)
    weights = softmax_weights(scores)
    values = value_part.reshape(source_count, head_count, HEAD_DIM)
    mixed = jnp.einsum("hqk,khd->qhd", weights, values, preferred_element_type=jnp.float32)
    return mixed.astype(jnp.bfloat16).reshape(query_count, width)


def project_attend(query_rows, source_rows, query_weight, keyval_weight):
    width = query_weight.shape[1]
    queries = jnp.dot(query_rows, query_weight, preferred_element_type=jnp.float32).astype(
        jnp.bfloat16
    )
    flat_weight = keyval_weight.reshape(keyval_weight.shape[0], 2 * width)
    keyvals = jnp.dot(source_rows, flat_weight, preferred_element_type=jnp.float32).astype(
        jnp.bfloat16
    )
    key_part = keyvals[:, :width]
    value_part = keyvals[:, width:]
    if width >= HEAD_DIM:
        return local_heads(queries, key_part, value_part)
    query_float = queries.astype(jnp.float32)
    key_float = key_part.astype(jnp.float32)
    query_square = jnp.sum(query_float * query_float, axis=1, keepdims=True)
    key_square = jnp.sum(key_float * key_float, axis=1, keepdims=True)
    other_query, other_key = partner((query_square, key_square), "tensor", 0)
    query_hat = (query_float * lax.rsqrt((query_square + other_query) / HEAD_DIM + epsilon)).astype(
        jnp.bfloat16
    )
    key_hat = (key_float * lax.rsqrt((key_square + other_key) / HEAD_DIM + epsilon)).astype(
        jnp.bfloat16
    )
    partial_scores = jnp.einsum("qd,kd->qk", query_hat, key_hat, preferred_element_type=jnp.float32)
    other_scores = partner(partial_scores, "tensor", 0)
    scores = (partial_scores + other_scores) * HEAD_DIM ** (-0.5)
    weights = softmax_weights(scores)
    return jnp.dot(weights, value_part, preferred_element_type=jnp.float32).astype(jnp.bfloat16)


def output_rows(mixed, weight):
    return jnp.dot(mixed, weight, preferred_element_type=jnp.float32)


def feed_rows(inputs, expand, shrink):
    hidden = jnp.dot(inputs, expand, preferred_element_type=jnp.float32)
    hidden = jax.nn.gelu(hidden, approximate=True).astype(jnp.bfloat16)
    return jnp.dot(hidden, shrink, preferred_element_type=jnp.float32)


def on_device(
    video_state,
    audio_state,
    video_modulation,
    audio_modulation,
    video_query,
    audio_keyval,
    video_output,
    audio_query,
    video_keyval,
    audio_output,
    video_expand,
    video_shrink,
    audio_expand,
    audio_shrink,
):
    video_count = video_state.shape[0]
    audio_own = modulate(audio_state, audio_modulation, 0)
    video_whole = lax.all_gather(video_state, "tensor", axis=0, tiled=True)
    video_normed = modulate(video_whole, video_modulation, 0)
    audio_normed = lax.all_gather(audio_own, "tensor", axis=0, tiled=True)
    video_mixed = project_attend(video_normed, audio_normed, video_query, audio_keyval)
    audio_mixed = project_attend(audio_normed, video_normed, audio_query, video_keyval)
    audio_term = lax.psum_scatter(
        output_rows(audio_mixed, audio_output), "tensor", scatter_dimension=0, tiled=True
    )
    audio_mid = audio_state + audio_modulation[2] * audio_term
    audio_inner_own = modulate(audio_mid, audio_modulation, 3)
    partial_term = jnp.dot(video_mixed, video_output, preferred_element_type=jnp.float32)
    full_term = lax.psum(partial_term, "tensor")
    video_mid_whole = video_whole + video_modulation[2] * full_term
    video_inner = modulate(video_mid_whole, video_modulation, 3)
    first_row = lax.axis_index("tensor") * video_count
    video_mid = lax.dynamic_slice_in_dim(video_mid_whole, first_row, video_count, 0)
    audio_inner = lax.all_gather(audio_inner_own, "tensor", axis=0, tiled=True)
    video_feed = lax.psum_scatter(
        feed_rows(video_inner, video_expand, video_shrink),
        "tensor",
        scatter_dimension=0,
        tiled=True,
    )
    audio_feed = lax.psum_scatter(
        feed_rows(audio_inner, audio_expand, audio_shrink),
        "tensor",
        scatter_dimension=0,
        tiled=True,
    )
    video_next = video_mid + video_modulation[5] * video_feed
    audio_next = audio_mid + audio_modulation[5] * audio_feed
    return (video_next, audio_next)


VMEM_BYTES = 66_000_000
WEIGHT_BYTES = 40 << 20


def matmul_to(lhs_ref, weight_ref, tile, emit):
    def body(i, carry):
        columns = pl.ds(pl.multiple_of(i * tile, tile), tile)
        emit(
            columns,
            jnp.dot(lhs_ref[...], weight_ref[:, columns], preferred_element_type=jnp.float32),
        )
        return carry

    lax.fori_loop(0, weight_ref.shape[1] // tile, body, 0)


class Stream:
    names = ("own", "slots", "wide", "whole", "other", "paired", "sums", "terms", "total")

    @staticmethod
    def scratch(count, rows, width):
        chips = count // 2
        return [
            pltpu.VMEM((rows, width), jnp.bfloat16),
            pltpu.VMEM((count, rows, width), jnp.bfloat16),
            pltpu.VMEM((chips, 2 * rows, width), jnp.float32),
            pltpu.VMEM((count * rows, width), jnp.bfloat16),
            pltpu.VMEM((chips, rows, width), jnp.bfloat16),
            pltpu.VMEM((chips, rows, width), jnp.bfloat16),
            pltpu.VMEM((chips, rows, width), jnp.bfloat16),
            pltpu.VMEM((chips, rows, width), jnp.bfloat16),
            pltpu.VMEM((rows, width), jnp.float32),
            pltpu.SemaphoreType.DMA((2 * chips,)),
            pltpu.SemaphoreType.DMA((count,)),
            pltpu.SemaphoreType.DMA((chips + 1,)),
            pltpu.SemaphoreType.DMA((chips + 1,)),
        ]

    def __init__(self, refs, count):
        for name, ref in zip(self.names, refs):
            setattr(self, name, ref)
        self.gather_send, self.gather_recv, self.scatter_send, self.scatter_recv = refs[len(self.names):]
        self.count, self.chips = count, count // 2
        self.rows = self.own.shape[0]
        self.me = lax.axis_index("tensor")
        self.chip, self.core = self.me // 2, self.me % 2
        self.mate = self.chip * 2 + (1 - self.core)

    def distant(self, step):
        return lax.rem(self.chip + step, self.chips)

    def to_mate(self, slot, source, send):
        return pltpu.make_async_remote_copy(
            src_ref=source,
            dst_ref=self.slots.at[slot],
            send_sem=self.gather_send.at[send],
            recv_sem=self.gather_recv.at[slot],
            device_id={"tensor": self.mate},
            device_id_type=pl.DeviceIdType.MESH,
        )

    def to_chip(self, step):
        return pltpu.make_async_remote_copy(
            src_ref=self.own,
            dst_ref=self.slots.at[self.me],
            send_sem=self.gather_send.at[step],
            recv_sem=self.gather_recv.at[self.me],
            device_id={"tensor": self.distant(step) * 2 + self.core},
            device_id_type=pl.DeviceIdType.MESH,
        )

    def keep(self):
        return pltpu.make_async_copy(self.own, self.slots.at[self.me], self.gather_recv.at[self.me])

    def gather_start(self):
        for step in range(self.chips - 1, 0, -1):
            self.to_chip(step).start()
        self.to_mate(self.me, self.own, 0).start()
        self.keep().start()

    def arrived(self, slot):
        pltpu.make_async_copy(self.slots.at[slot], self.slots.at[slot], self.gather_recv.at[slot]).wait()

    def gather_forward(self):
        for step in range(1, self.chips):
            slot = self.distant(step) * 2 + self.core
            self.arrived(slot)
            self.to_mate(slot, self.slots.at[slot], self.chips + step).start()

    def gather_finish(self):
        self.keep().wait()
        for step in range(self.chips):
            self.arrived(self.distant(step) * 2 + 1 - self.core)

        def widen(chip, carry):
            self.wide[chip, : self.rows, :] = self.slots[2 * chip].astype(jnp.float32)
            self.wide[chip, self.rows :, :] = self.slots[2 * chip + 1].astype(jnp.float32)
            return carry

        lax.fori_loop(0, self.chips, widen, 0)
        self.whole[...] = self.wide[...].reshape(self.whole.shape).astype(jnp.bfloat16)

    def gather_drain(self):
        for step in range(1, self.chips):
            slot = self.distant(step) * 2 + self.core
            self.to_chip(step).wait_send()
            self.to_mate(slot, self.slots.at[slot], self.chips + step).wait_send()
        self.to_mate(self.me, self.own, 0).wait_send()

    def emit(self, columns, product):
        self.wide[:, :, columns] = product.reshape(self.chips, 2 * self.rows, product.shape[1])

    def swap(self):
        return pltpu.make_async_remote_copy(
            src_ref=self.other,
            dst_ref=self.paired,
            send_sem=self.scatter_send.at[self.chips],
            recv_sem=self.scatter_recv.at[self.chips],
            device_id={"tensor": self.mate},
            device_id_type=pl.DeviceIdType.MESH,
        )

    def halves(self, chip):
        rows = self.wide[chip]
        low, high = rows[: self.rows], rows[self.rows :]
        first = self.core == 0
        return jnp.where(first, low, high), jnp.where(first, high, low)

    def scatter_start(self):
        def body(chip, carry):
            self.other[chip] = self.halves(chip)[1].astype(jnp.bfloat16)
            return carry

        lax.fori_loop(0, self.chips, body, 0)
        self.swap().start()

    def term(self, step):
        goal = self.distant(step)
        return pltpu.make_async_remote_copy(
            src_ref=self.sums.at[goal],
            dst_ref=self.terms.at[self.chip],
            send_sem=self.scatter_send.at[step],
            recv_sem=self.scatter_recv.at[self.chip],
            device_id={"tensor": goal * 2 + self.core},
            device_id_type=pl.DeviceIdType.MESH,
        )

    def scatter_send_on(self):
        self.swap().wait()
        for step in range(1, self.chips):
            goal = self.distant(step)
            self.sums[goal] = (
                self.halves(goal)[0] + self.paired[goal].astype(jnp.float32)
            ).astype(jnp.bfloat16)
            self.term(step).start()
        self.total[...] = self.halves(self.chip)[0] + self.paired[self.chip].astype(jnp.float32)

    def scatter_finish(self):
        for step in range(1, self.chips):
            source = self.distant(step)
            pltpu.make_async_copy(
                self.terms.at[source], self.terms.at[source], self.scatter_recv.at[source]
            ).wait()
            self.total[...] += self.terms[source].astype(jnp.float32)
        for step in range(1, self.chips):
            self.term(step).wait_send()
        return self.total[...]


def split_pairs(pairs_ref, wide_ref, even_ref, odd_ref, rows):
    def body(i, carry):
        start = pl.multiple_of(i * rows, rows)
        wide_ref[...] = pairs_ref[pl.ds(pl.multiple_of(i * 2 * rows, 2 * rows), 2 * rows), :].astype(
            jnp.float32
        )
        even_ref[pl.ds(start, rows), :] = wide_ref[pl.ds(0, rows, stride=2), :].astype(jnp.bfloat16)
        odd_ref[pl.ds(start, rows), :] = wide_ref[pl.ds(1, rows, stride=2), :].astype(jnp.bfloat16)
        return carry

    lax.fori_loop(0, even_ref.shape[0] // rows, body, 0)


def segment_normalize(tensor):
    values = tensor.astype(jnp.float32)
    squares = values * values
    head_of = lax.broadcasted_iota(jnp.int32, values.shape, 1) // HEAD_DIM
    scale = jnp.zeros_like(values)
    for head in range(values.shape[1] // HEAD_DIM):
        mine = head_of == head
        mean = jnp.sum(jnp.where(mine, squares, 0.0), axis=-1, keepdims=True) / HEAD_DIM
        scale = jnp.where(mine, lax.rsqrt(mean + epsilon), scale)
    return values * scale


def attend(queries, keys, values):
    query_hat = segment_normalize(queries)
    key_hat = segment_normalize(keys).astype(jnp.bfloat16)
    head_of = lax.broadcasted_iota(jnp.int32, query_hat.shape, 1) // HEAD_DIM
    mixed = jnp.zeros(query_hat.shape, jnp.float32)
    for head in range(query_hat.shape[1] // HEAD_DIM):
        mine = head_of == head
        own = jnp.where(mine, query_hat, 0.0).astype(jnp.bfloat16)
        scores = lax.dot_general(
            own, key_hat, (((1,), (1,)), ((), ())), preferred_element_type=jnp.float32
        ) * HEAD_DIM ** (-0.5)
        weights = softmax_weights(scores)
        mixed = jnp.where(mine, jnp.dot(weights, values, preferred_element_type=jnp.float32), mixed)
    return mixed.astype(jnp.bfloat16)


def modulate_rows(states, modulation_ref, first):
    normed = states * lax.rsqrt(jnp.mean(states * states, axis=-1, keepdims=True) + epsilon)
    return (
        normed * (1.0 + modulation_ref[first + 1 : first + 2, :]) + modulation_ref[first : first + 1, :]
    ).astype(jnp.bfloat16)


def project(rows_ref, weight_ref):
    return jnp.dot(rows_ref[...], weight_ref[...], preferred_element_type=jnp.float32).astype(jnp.bfloat16)


def block_kernel(count, video_width, audio_width, *refs):
    video_state, audio_state, video_mod, audio_mod = refs[:4]
    weights_hbm = refs[4:14]
    video_out, audio_out = refs[14:16]
    weights = refs[16:26]
    rest = refs[26:]
    size = 13
    video1, audio1, video2, audio2 = (
        Stream(rest[i * size : (i + 1) * size], count) for i in range(4)
    )
    (weight_sem, pair_wide, video_key, video_value, audio_key, audio_value,
     video_mixed, audio_mixed, video_hidden, audio_hidden) = rest[4 * size :]
    loads = [
        pltpu.make_async_copy(hbm, vmem, weight_sem.at[i])
        for i, (hbm, vmem) in enumerate(zip(weights_hbm, weights))
    ]
    (audio_query, audio_pairs, video_query, video_pairs, audio_output, video_output,
     audio_expand, audio_shrink, video_expand, video_shrink) = weights
    for load in loads:
        load.start()

    barrier = pltpu.get_barrier_semaphore()
    for step in range(1, video1.chips):
        pl.semaphore_signal(
            barrier,
            inc=1,
            device_id={"tensor": video1.distant(step) * 2 + video1.core},
            device_id_type=pl.DeviceIdType.MESH,
        )
    pl.semaphore_signal(
        barrier, inc=1, device_id={"tensor": video1.mate}, device_id_type=pl.DeviceIdType.MESH
    )
    audio1.own[...] = modulate_rows(audio_state[...], audio_mod, 0)
    video1.own[...] = modulate_rows(video_state[...], video_mod, 0)
    pl.semaphore_wait(barrier, video1.chips)

    audio1.gather_start()
    video1.gather_start()
    loads[1].wait()
    split_pairs(audio_pairs, pair_wide, audio_key, audio_value, pair_wide.shape[0] // 2)
    audio1.gather_forward()
    loads[3].wait()
    split_pairs(video_pairs, pair_wide, video_key, video_value, pair_wide.shape[0] // 2)
    audio1.gather_finish()
    loads[0].wait()
    audio_queries = project(audio1.whole, audio_query)
    audio_keys = project(audio1.whole, audio_key)
    audio_values = project(audio1.whole, audio_value)
    video1.gather_forward()
    video1.gather_finish()
    loads[2].wait()
    video_keys = project(video1.whole, video_key)
    video_values = project(video1.whole, video_value)
    audio_mixed[...] = attend(audio_queries, video_keys, video_values)
    loads[4].wait()
    matmul_to(audio_mixed, audio_output, 512, audio1.emit)
    audio1.scatter_start()
    video_queries = project(video1.whole, video_query)
    video_mixed[...] = attend(video_queries, audio_keys, audio_values)
    audio1.scatter_send_on()
    loads[5].wait()
    matmul_to(video_mixed, video_output, 512, video1.emit)
    video1.scatter_start()
    audio1.gather_drain()
    video1.gather_drain()
    video1.scatter_send_on()
    audio_mid = audio_state[...] + audio_mod[2:3, :] * audio1.scatter_finish()
    audio_out[...] = audio_mid
    audio2.own[...] = modulate_rows(audio_mid, audio_mod, 3)
    audio2.gather_start()
    video_mid = video_state[...] + video_mod[2:3, :] * video1.scatter_finish()
    video_out[...] = video_mid
    video2.own[...] = modulate_rows(video_mid, video_mod, 3)
    video2.gather_start()
    audio2.gather_forward()
    audio2.gather_finish()

    def keep_hidden(target):
        def emit(columns, product):
            target[:, columns] = jax.nn.gelu(product, approximate=True).astype(jnp.bfloat16)

        return emit

    loads[6].wait()
    matmul_to(audio2.whole, audio_expand, 256, keep_hidden(audio_hidden))
    loads[7].wait()
    matmul_to(audio_hidden, audio_shrink, 512, audio2.emit)
    audio2.scatter_start()
    video2.gather_forward()
    audio2.scatter_send_on()
    video2.gather_finish()
    loads[8].wait()
    matmul_to(video2.whole, video_expand, 256, keep_hidden(video_hidden))
    loads[9].wait()
    matmul_to(video_hidden, video_shrink, 512, video2.emit)
    video2.scatter_start()
    audio_out[...] += audio_mod[5:6, :] * audio2.scatter_finish()
    audio2.gather_drain()
    video2.gather_drain()
    video2.scatter_send_on()
    video_out[...] += video_mod[5:6, :] * video2.scatter_finish()


def hand_over(video_ref, audio_ref, video_out, audio_out):
    video_out[...] = video_ref[...]
    audio_out[...] = audio_ref[...]


def fused_block(
    video_state,
    audio_state,
    video_modulation,
    audio_modulation,
    video_query,
    audio_keyval,
    video_output,
    audio_query,
    video_keyval,
    audio_output,
    video_expand,
    video_shrink,
    audio_expand,
    audio_shrink,
):
    count = lax.axis_size("tensor")
    rows, video_width = video_state.shape
    audio_width = audio_state.shape[1]
    width = video_query.shape[1]
    tokens = count * rows
    weights = (
        audio_query,
        audio_keyval.reshape(-1, width),
        video_query,
        video_keyval.reshape(-1, width),
        audio_output,
        video_output,
        audio_expand,
        audio_shrink,
        video_expand,
        video_shrink,
    )
    vmem = pl.BlockSpec(memory_space=pltpu.VMEM)
    hbm = pl.BlockSpec(memory_space=pl.ANY)
    streams = []
    for extent in (video_width, audio_width) * 2:
        streams += Stream.scratch(count, rows, extent)
    bf16 = jnp.bfloat16
    results = (
        jax.ShapeDtypeStruct(video_state.shape, jnp.float32),
        jax.ShapeDtypeStruct(audio_state.shape, jnp.float32),
    )
    video_next, audio_next = pl.pallas_call(
        functools.partial(block_kernel, count, video_width, audio_width),
        out_shape=results,
        in_specs=[vmem] * 4 + [hbm] * len(weights),
        out_specs=(vmem, vmem),
        scratch_shapes=[pltpu.VMEM(weight.shape, weight.dtype) for weight in weights]
        + streams
        + [
            pltpu.SemaphoreType.DMA((len(weights),)),
            pltpu.VMEM((512, width), jnp.float32),
            pltpu.VMEM((video_width, width), bf16),
            pltpu.VMEM((video_width, width), bf16),
            pltpu.VMEM((audio_width, width), bf16),
            pltpu.VMEM((audio_width, width), bf16),
            pltpu.VMEM((tokens, width), bf16),
            pltpu.VMEM((tokens, width), bf16),
            pltpu.VMEM((tokens, video_expand.shape[1]), bf16),
            pltpu.VMEM((tokens, audio_expand.shape[1]), bf16),
        ],
        compiler_params=pltpu.CompilerParams(
            collective_id=0, has_side_effects=True, vmem_limit_bytes=VMEM_BYTES
        ),
    )(video_state, audio_state, video_modulation, audio_modulation, *weights)
    return pl.pallas_call(
        hand_over, out_shape=results, in_specs=[vmem] * 2, out_specs=(vmem, vmem)
    )(video_next, audio_next)


def block(*arrays):
    count = lax.axis_size("tensor")
    rows = arrays[0].shape[0]
    width = arrays[4].shape[1]
    held = sum(array.size * array.dtype.itemsize for array in arrays[4:])
    fits = held <= WEIGHT_BYTES and count * rows <= 64
    shaped = count % 2 == 0 and 2 * rows % 8 == 0 and width % 128 == 0
    tiled = all(array.shape[1] % 512 == 0 for array in arrays[:2]) and all(
        arrays[i].shape[1] % 256 == 0 for i in (10, 12)
    )
    return fused_block(*arrays) if fits and shaped and tiled else on_device(*arrays)


def solution(mesh):
    placed = (
        P(("groups", "tensor"), None),
        P(("groups", "tensor"), None),
        P("groups", None),
        P("groups", None),
        P(None, "tensor"),
        P(None, None, "tensor"),
        P("tensor", None),
        P(None, "tensor"),
        P(None, None, "tensor"),
        P("tensor", None),
        P(None, "tensor"),
        P("tensor", None),
        P(None, "tensor"),
        P("tensor", None),
    )
    return jax.shard_map(
        block,
        mesh=mesh,
        in_specs=placed,
        out_specs=(P(("groups", "tensor"), None), P(("groups", "tensor"), None)),
        check_vma=False,
    )
```
